16 devices in a mesh: dp: 1, tp: 16 (over x, y, z, core).
Axes of the slice: x: 2, y: 2, z: 2, core: 2. Of those that a mesh axis runs over, the one named last changes fastest.
Arguments:
- x: bfloat16 [2048, 3072], P('dp')
- dy: bfloat16 [2048, 3072], P('dp')
- gate: bfloat16 [2048, 8192], P('dp', 'tp')
- up: bfloat16 [2048, 8192], P('dp', 'tp')
- w_gate: bfloat16 [3072, 8192], P(None, 'tp')
- w_up: bfloat16 [3072, 8192], P(None, 'tp')
- w_down: bfloat16 [8192, 3072], P('tp')
Outputs:
- output 1: bfloat16 [2048, 3072], P('dp')
- output 2: bfloat16 [3072, 8192], P('dp', 'tp')
- output 3: bfloat16 [3072, 8192], P('dp', 'tp')
- output 4: bfloat16 [8192, 3072], P(('dp', 'tp'))
All inputs are finite; a program needn't handle non-finite values.
Results may differ from the reference program's by a relative error of at most 0.012.
Values are sent between devices in bfloat16 or wider.
A program may use at most 2 GiB of HBM per device.

```python
import jax
import jax.numpy as jnp

ROWS = 2048
D = 3072
FF = 8192


def act(gate, up):
    return jax.nn.silu(gate) * up


def setup_inputs(seed: int = 0, part: int = 0) -> dict:
    kx, ky, ka, kb, kg, ku, kd = jax.random.split(jax.random.key(seed), 7)
    kx, ky, ka, kb = (jax.random.fold_in(k, part) for k in (kx, ky, ka, kb))
    drawn = {
        "x": jax.random.normal(kx, (ROWS, D), jnp.float32),
        "dy": jax.random.normal(ky, (ROWS, D), jnp.float32),
        "gate": jax.random.normal(ka, (ROWS, FF), jnp.float32),
        "up": jax.random.normal(kb, (ROWS, FF), jnp.float32),
        "w_gate": jax.random.normal(kg, (D, FF), jnp.float32) * D**-0.5,
        "w_up": jax.random.normal(ku, (D, FF), jnp.float32) * D**-0.5,
        "w_down": jax.random.normal(kd, (FF, D), jnp.float32) * FF**-0.5,
    }
    return {k: v.astype(jnp.bfloat16) for k, v in drawn.items()}


def reference(x, dy, gate, up, w_gate, w_up, w_down):
    hidden, back = jax.vjp(act, gate.astype(jnp.float32), up.astype(jnp.float32))
    d_hidden = jnp.dot(dy, w_down.T, preferred_element_type=jnp.float32)
    d_gate, d_up = (g.astype(jnp.bfloat16) for g in back(d_hidden))
    dx = jnp.dot(d_gate, w_gate.T, preferred_element_type=jnp.float32) + jnp.dot(d_up, w_up.T, preferred_element_type=jnp.float32)
    dw_gate = jnp.dot(x.T, d_gate, preferred_element_type=jnp.float32)
    dw_up = jnp.dot(x.T, d_up, preferred_element_type=jnp.float32)
    dw_down = jnp.dot(hidden.astype(jnp.bfloat16).T, dy, preferred_element_type=jnp.float32)
    return tuple(g.astype(jnp.bfloat16) for g in (dx, dw_gate, dw_up, dw_down))
```

```python
import functools

import jax
import jax.numpy as jnp
from jax import lax
from jax.experimental import pallas as pl
from jax.experimental.pallas import tpu as pltpu
from jax.sharding import PartitionSpec as P

MESH = pl.DeviceIdType.MESH
CHUNKS = 8
TILE = 256
ORDERS = ((8, 4, 2), (4, 2, 8), (2, 8, 4))


def dot_nt(a, b):
    return lax.dot_general(a, b, (((1,), (1,)), ((), ())), preferred_element_type=jnp.float32)


def dot_tn(a, b):
    return lax.dot_general(a, b, (((0,), (0,)), ((), ())), preferred_element_type=jnp.float32)


def kernel(
    x, dy, gate, up, wg, wu, wdn, dx, dwg, dwu, dwd,
    wgu, wd, dyb, gb, ub, d, hid_t, own, s0, s1, s2, s3, r0, r1, r2, r3, xb, yb, og, od,
    w_sem, in_sem, xy_sem, out_sem, s_sems, r_sems, ag_send, fwd_send, fwd_recv,
):
    rows, width = dx.shape
    ff = gate.shape[1]
    R = rows // CHUNKS
    C = width // 6
    dp = lax.axis_index("dp")
    me = lax.axis_index("tp")
    core = lax.rem(me, 2)
    mate = me + 1 - 2 * core
    bits = {s: lax.rem(me // s, 2) for s in (2, 4, 8)}
    peer = {s: me + (1 - 2 * bits[s]) * s for s in (2, 4, 8)}
    units = width // TILE

    def fetch(t):
        sl = lax.rem(t, 2)
        r = pl.ds(t * R, R)
        return (
            pltpu.make_async_copy(dy.at[r, :], dyb.at[sl], in_sem.at[0, sl]),
            pltpu.make_async_copy(gate.at[r, :], gb.at[sl], in_sem.at[1, sl]),
            pltpu.make_async_copy(up.at[r, :], ub.at[sl], in_sem.at[2, sl]),
        )

    def fetch_cols(u):
        sl = lax.rem(u, 2)
        c = pl.ds(pl.multiple_of(u * TILE, TILE), TILE)
        return (
            pltpu.make_async_copy(x.at[:, c], xb.at[sl], xy_sem.at[0, sl]),
            pltpu.make_async_copy(dy.at[:, c], yb.at[sl], xy_sem.at[1, sl]),
        )

    def put(u):
        sl = lax.rem(u, 2)
        c = pl.ds(pl.multiple_of(u * TILE, TILE), TILE)
        return (
            pltpu.make_async_copy(og.at[sl, :, pl.ds(0, ff)], dwg.at[c, :], out_sem.at[0, sl]),
            pltpu.make_async_copy(og.at[sl, :, pl.ds(ff, ff)], dwu.at[c, :], out_sem.at[1, sl]),
            pltpu.make_async_copy(od.at[sl], dwd.at[:, c], out_sem.at[2, sl]),
        )

    weights = (
        pltpu.make_async_copy(wdn, wd, w_sem.at[0]),
        pltpu.make_async_copy(wg, wgu.at[:, pl.ds(0, ff)], w_sem.at[1]),
        pltpu.make_async_copy(wu, wgu.at[:, pl.ds(ff, ff)], w_sem.at[2]),
    )
    weights[0].start()
    for c in fetch(0):
        c.start()
    weights[1].start()
    weights[2].start()

    barrier = pltpu.get_barrier_semaphore()
    for to in (mate, peer[2], peer[4], peer[8]):
        pl.semaphore_signal(barrier, inc=1, device_id=(dp, to), device_id_type=MESH)
    pl.semaphore_wait(barrier, 4)
    weights[0].wait()

    def halves(p):
        n, kept, out = R, 0, []
        for s in ORDERS[p]:
            n //= 2
            out.append((n, kept + bits[s] * n, kept + (1 - bits[s]) * n, s))
            kept = kept + bits[s] * n
        return out

    def remote(src, dst, send, recv, to):
        return pltpu.make_async_remote_copy(
            src_ref=src, dst_ref=dst, send_sem=send, recv_sem=recv, device_id=(dp, to), device_id_type=MESH
        )

    sends, recvs = (s0, s1, s2, s3), (r0, r1, r2, r3)

    def reduce_copy(stage, k, p):
        sl = lax.rem(k, 2)
        to = mate if stage == 0 else peer[ORDERS[p][stage - 1]]
        return remote(
            sends[stage].at[sl, p], recvs[stage].at[k, p], s_sems.at[stage, sl, p], r_sems.at[stage, k, p], to
        )

    def out_slice(k, p, off, n, c):
        row = pl.multiple_of(k * R + off, n)
        col = pl.multiple_of(p * 2 * C + c * C, C)
        return dx.at[pl.ds(row, n), pl.ds(col, C)]

    def gather_copy(stage, k, p):
        n, kept, _, s = halves(p)[2 - stage]
        ref = out_slice(k, p, kept, n, core)
        return remote(ref, ref, ag_send, r_sems.at[4 + stage, k, p], peer[s])

    def forward_copy(k, p, off, n):
        ref = out_slice(k, p, off, n, core)
        return remote(ref, ref, fwd_send, fwd_recv, mate)

    def partial(k, p, stage, off, n):
        hs = halves(p)
        sl = lax.rem(k, 4)
        total = own[sl, p, pl.ds(pl.multiple_of(off, n), n), :]
        base = 0
        for i in range(stage):
            total += recvs[i][k, p, pl.ds(pl.multiple_of(off - base, n), n), :].astype(jnp.float32)
            base = hs[i][1] if i < 3 else base
        return total

    def reduce_step(stage, k):
        sl = lax.rem(k, 2)

        @pl.when(k >= 2)
        def _():
            for p in range(3):
                reduce_copy(stage, k - 2, p).wait_send()

        for p in range(3):
            n, _, sent, _ = halves(p)[stage - 1]
            reduce_copy(stage - 1, k, p).wait_recv()
            sends[stage][sl, p] = partial(k, p, stage, sent, n).astype(jnp.bfloat16)
            reduce_copy(stage, k, p).start()

    def finish_step(k):
        for p in range(3):
            n, kept, _, _ = halves(p)[2]
            reduce_copy(3, k, p).wait_recv()
            row = pl.multiple_of(k * R + kept, n)
            col = pl.multiple_of(p * 2 * C + core * C, C)
            dx[pl.ds(row, n), pl.ds(col, C)] = partial(k, p, 4, kept, n).astype(jnp.bfloat16)
            gather_copy(0, k, p).start()
            forward_copy(k, p, kept, n).start()

    def gather_step(stage, k):
        for p in range(3):
            n, _, other, _ = halves(p)[3 - stage]
            gather_copy(stage - 1, k, p).wait_recv()
            if stage < 3:
                gather_copy(stage, k, p).start()
            forward_copy(k, p, other, n).start()

    def live(t, lag, f):
        k = t - lag

        @pl.when((k >= 0) & (k < CHUNKS))
        def _():
            f(k)

    def hidden_grads(t):
        sl = lax.rem(t, 2)
        for c in fetch(t):
            c.wait()
        r = pl.ds(pl.multiple_of(t * R, R), R)
        step = ff // 2
        for h in range(2):
            c = pl.ds(h * step, step)
            dh = dot_nt(dyb[sl], wd[c, :])
            g = gb[sl, :, c].astype(jnp.float32)
            u = ub[sl, :, c].astype(jnp.float32)
            sg = jax.nn.sigmoid(g)
            silu = g * sg
            d[r, pl.ds(ff + h * step, step)] = (dh * silu).astype(jnp.bfloat16)
            d[r, c] = ((dh * u) * (sg * (1.0 + g * (1.0 - sg)))).astype(jnp.bfloat16)
            hid_t[c, r] = (silu * u).astype(jnp.bfloat16).T

        @pl.when(t + 1 < CHUNKS)
        def _():
            for c in fetch(t + 1):
                c.start()

    def terms(t):
        sl = lax.rem(t, 2)
        r = pl.ds(pl.multiple_of(t * R, R), R)

        @pl.when(t >= 2)
        def _():
            for p in range(3):
                reduce_copy(0, t - 2, p).wait_send()

        for p in range(3):
            w = pl.ds(pl.multiple_of(p * 2 * C + (1 - core) * C, C), C)
            s0[sl, p] = dot_nt(d[r, :], wgu[w, :]).astype(jnp.bfloat16)
            reduce_copy(0, t, p).start()
        for p in range(3):
            w = pl.ds(pl.multiple_of(p * 2 * C + core * C, C), C)
            own[lax.rem(t, 4), p] = dot_nt(d[r, :], wgu[w, :])

    def weight_grads(u):
        sl = lax.rem(u, 2)

        @pl.when(u >= 2)
        def _():
            for c in put(u - 2):
                c.wait()

        for c in fetch_cols(u):
            c.wait()
        og[sl] = dot_tn(xb[sl], d[...]).astype(jnp.bfloat16)
        od[sl] = jnp.dot(hid_t[...], yb[sl], preferred_element_type=jnp.float32).astype(jnp.bfloat16)
        for c in put(u):
            c.start()

        @pl.when(u + 2 < units)
        def _():
            for c in fetch_cols(u + 2):
                c.start()

    def step(t, _):
        @pl.when(t < CHUNKS)
        def _():
            hidden_grads(t)

        @pl.when(t == 0)
        def _():
            weights[1].wait()
            weights[2].wait()
            for u in range(2):
                for c in fetch_cols(u):
                    c.start()

        @pl.when((t >= CHUNKS) & (2 * (t - CHUNKS) < units))
        def _():
            weight_grads(2 * (t - CHUNKS))

        live(t, 1, lambda k: reduce_step(1, k))
        live(t, 2, lambda k: reduce_step(2, k))
        live(t, 3, lambda k: reduce_step(3, k))
        live(t, 4, finish_step)

        @pl.when(t < CHUNKS)
        def _():
            terms(t)

        live(t, 5, lambda k: gather_step(1, k))
        live(t, 6, lambda k: gather_step(2, k))
        live(t, 7, lambda k: gather_step(3, k))

        @pl.when((t >= CHUNKS) & (2 * (t - CHUNKS) < units))
        def _():
            weight_grads(2 * (t - CHUNKS) + 1)

        return 0

    lax.fori_loop(0, CHUNKS + 7, step, 0)

    for u in (units - 2, units - 1):
        for c in put(u):
            c.wait()
    for stage in range(4):
        for k in (CHUNKS - 2, CHUNKS - 1):
            for p in range(3):
                reduce_copy(stage, k, p).wait_send()
    part = dx.at[pl.ds(0, rows // 8 * 7), pl.ds(0, width // 2)]
    remote(part, part, ag_send, fwd_recv, mate).wait_send()
    half = dx.at[:, pl.ds(0, width // 2)]
    remote(half, half, fwd_send, fwd_recv, mate).wait()


def solution(mesh):
    def step(x, dy, gate, up, w_gate, w_up, w_down):
        rows, width = dy.shape
        ff = gate.shape[1]
        R, C, K = rows // CHUNKS, width // 6, CHUNKS
        bf, f32 = jnp.bfloat16, jnp.float32
        V, D = pltpu.VMEM, pltpu.SemaphoreType.DMA
        flops = 2 * rows * width * ff * 6
        hbm = pl.BlockSpec(memory_space=pl.ANY)
        return pl.pallas_call(
            kernel,
            out_shape=(
                jax.ShapeDtypeStruct((rows, width), bf),
                jax.ShapeDtypeStruct((width, ff), bf),
                jax.ShapeDtypeStruct((width, ff), bf),
                jax.ShapeDtypeStruct((ff, width), bf),
            ),
            in_specs=[hbm] * 7,
            out_specs=(pl.BlockSpec(memory_space=pltpu.VMEM), hbm, hbm, hbm),
            scratch_shapes=[
                V((width, 2 * ff), bf), V((ff, width), bf),
                V((2, R, width), bf), V((2, R, ff), bf), V((2, R, ff), bf),
                V((rows, 2 * ff), bf), V((ff, rows), bf),
                V((4, 3, R, C), f32),
                V((2, 3, R, C), bf), V((2, 3, R // 2, C), bf), V((2, 3, R // 4, C), bf), V((2, 3, R // 8, C), bf),
                V((K, 3, R, C), bf), V((K, 3, R // 2, C), bf), V((K, 3, R // 4, C), bf), V((K, 3, R // 8, C), bf),
                V((2, rows, TILE), bf), V((2, rows, TILE), bf),
                V((2, TILE, 2 * ff), bf), V((2, ff, TILE), bf),
                D((3,)), D((3, 2)), D((2, 2)), D((3, 2)), D((4, 2, 3)), D((7, K, 3)), D, D, D,
            ],
            compiler_params=pltpu.CompilerParams(
                collective_id=0, has_side_effects=True, vmem_limit_bytes=67_043_328
            ),
            cost_estimate=pl.CostEstimate(flops=flops, bytes_accessed=60_000_000, transcendentals=rows * ff),
            name="mlp_grads",
        )(x, dy, gate, up, w_gate, w_up, w_down)

    tokens, columns, rows = P("dp", None), P(None, "tp"), P("tp", None)
    return jax.shard_map(
        step,
        mesh=mesh,
        in_specs=(tokens, tokens, P("dp", "tp"), P("dp", "tp"), columns, columns, rows),
        out_specs=(tokens, P("dp", "tp"), P("dp", "tp"), P(("dp", "tp"), None)),
        check_vma=False,
    )
```

```python
import functools

import jax
import jax.numpy as jnp
from jax import lax
from jax.experimental import pallas as pl
from jax.experimental.pallas import tpu as pltpu
from jax.sharding import PartitionSpec as P

MESH = pl.DeviceIdType.MESH
CHUNKS = 8
TILE = 256
ORDERS = ((8, 4, 2), (4, 2, 8), (2, 8, 4))


def dot_nt(a, b):
    return lax.dot_general(a, b, (((1,), (1,)), ((), ())), preferred_element_type=jnp.float32)


def dot_tn(a, b):
    return lax.dot_general(a, b, (((0,), (0,)), ((), ())), preferred_element_type=jnp.float32)


def kernel(
    x, dy, gate, up, wg, wu, wdn, dx, dwg, dwu, dwd,
    dyb, gb, ub, d, hid_t, own, s0, s1, s2, s3, r0, r1, r2, r3, xb, yb,
    w_sem, in_sem, xy_sem, s_sems, r_sems, ag_send, fwd_send, fwd_recv,
):
    rows, width = dy.shape
    ff = gate.shape[1]
    R = rows // CHUNKS
    C = width // 6
    dp = lax.axis_index("dp")
    me = lax.axis_index("tp")
    core = lax.rem(me, 2)
    mate = me + 1 - 2 * core
    bits = {s: lax.rem(me // s, 2) for s in (2, 4, 8)}
    peer = {s: me + (1 - 2 * bits[s]) * s for s in (2, 4, 8)}
    units = width // TILE

    def fetch(t):
        sl = lax.rem(t, 2)
        r = pl.ds(t * R, R)
        return (
            pltpu.make_async_copy(dy.at[r, :], dyb.at[sl], in_sem.at[0, sl]),
            pltpu.make_async_copy(gate.at[r, :], gb.at[sl], in_sem.at[1, sl]),
            pltpu.make_async_copy(up.at[r, :], ub.at[sl], in_sem.at[2, sl]),
        )

    def fetch_cols(u):
        sl = lax.rem(u, 2)
        c = pl.ds(pl.multiple_of(u * TILE, TILE), TILE)
        return (
            pltpu.make_async_copy(x.at[:, c], xb.at[sl], xy_sem.at[0, sl]),
            pltpu.make_async_copy(dy.at[:, c], yb.at[sl], xy_sem.at[1, sl]),
        )

    weights = (
        pltpu.make_async_copy(wdn, dwd, w_sem.at[0]),
        pltpu.make_async_copy(wg, dwg, w_sem.at[1]),
        pltpu.make_async_copy(wu, dwu, w_sem.at[2]),
    )
    weights[0].start()
    for c in fetch(0):
        c.start()
    weights[1].start()
    weights[2].start()

    barrier = pltpu.get_barrier_semaphore()
    for to in (mate, peer[2], peer[4], peer[8]):
        pl.semaphore_signal(barrier, inc=1, device_id=(dp, to), device_id_type=MESH)
    pl.semaphore_wait(barrier, 4)
    weights[0].wait()

    def halves(p):
        n, kept, out = R, 0, []
        for s in ORDERS[p]:
            n //= 2
            out.append((n, kept + bits[s] * n, kept + (1 - bits[s]) * n, s))
            kept = kept + bits[s] * n
        return out

    def remote(src, dst, send, recv, to):
        return pltpu.make_async_remote_copy(
            src_ref=src, dst_ref=dst, send_sem=send, recv_sem=recv, device_id=(dp, to), device_id_type=MESH
        )

    sends, recvs = (s0, s1, s2, s3), (r0, r1, r2, r3)

    def reduce_copy(stage, k, p):
        sl = lax.rem(k, 2)
        to = mate if stage == 0 else peer[ORDERS[p][stage - 1]]
        return remote(
            sends[stage].at[sl, p], recvs[stage].at[k, p], s_sems.at[stage, sl, p], r_sems.at[stage, k, p], to
        )

    def out_slice(k, p, off, n, c):
        row = pl.multiple_of(k * R + off, n)
        return dx.at[2 * p + c, pl.ds(row, n), :]

    def gather_copy(stage, k, p):
        n, kept, _, s = halves(p)[2 - stage]
        ref = out_slice(k, p, kept, n, core)
        return remote(ref, ref, ag_send, r_sems.at[4 + stage, k, p], peer[s])

    def forward_copy(k, p, off, n):
        ref = out_slice(k, p, off, n, core)
        return remote(ref, ref, fwd_send, fwd_recv, mate)

    def partial(k, p, stage, off, n):
        hs = halves(p)
        sl = lax.rem(k, 4)
        total = own[sl, p, pl.ds(pl.multiple_of(off, n), n), :]
        base = 0
        for i in range(stage):
            total += recvs[i][k, p, pl.ds(pl.multiple_of(off - base, n), n), :].astype(jnp.float32)
            base = hs[i][1] if i < 3 else base
        return total

    def reduce_step(stage, k):
        sl = lax.rem(k, 2)

        @pl.when(k >= 2)
        def _():
            for p in range(3):
                reduce_copy(stage, k - 2, p).wait_send()

        for p in range(3):
            n, _, sent, _ = halves(p)[stage - 1]
            reduce_copy(stage - 1, k, p).wait_recv()
            sends[stage][sl, p] = partial(k, p, stage, sent, n).astype(jnp.bfloat16)
            reduce_copy(stage, k, p).start()

    def finish_step(k):
        for p in range(3):
            n, kept, _, _ = halves(p)[2]
            reduce_copy(3, k, p).wait_recv()
            row = pl.multiple_of(k * R + kept, n)
            dx[2 * p + core, pl.ds(row, n), :] = partial(k, p, 4, kept, n).astype(jnp.bfloat16)
            gather_copy(0, k, p).start()
            forward_copy(k, p, kept, n).start()

    def gather_step(stage, k):
        for p in range(3):
            n, _, other, _ = halves(p)[3 - stage]
            gather_copy(stage - 1, k, p).wait_recv()
            if stage < 3:
                gather_copy(stage, k, p).start()
            forward_copy(k, p, other, n).start()

    def live(t, lag, f):
        k = t - lag

        @pl.when((k >= 0) & (k < CHUNKS))
        def _():
            f(k)

    def hidden_grads(t):
        sl = lax.rem(t, 2)
        for c in fetch(t):
            c.wait()
        r = pl.ds(pl.multiple_of(t * R, R), R)
        step = ff // 2
        for h in range(2):
            c = pl.ds(h * step, step)
            dh = dot_nt(dyb[sl], dwd[c, :])
            g = gb[sl, :, c].astype(jnp.float32)
            u = ub[sl, :, c].astype(jnp.float32)
            sg = jax.nn.sigmoid(g)
            silu = g * sg
            d[r, pl.ds(ff + h * step, step)] = (dh * silu).astype(jnp.bfloat16)
            d[r, c] = ((dh * u) * (sg * (1.0 + g * (1.0 - sg)))).astype(jnp.bfloat16)
            hid_t[c, r] = (silu * u).astype(jnp.bfloat16).T

        @pl.when(t + 1 < CHUNKS)
        def _():
            for c in fetch(t + 1):
                c.start()

    def term(r, w):
        return dot_nt(d[r, pl.ds(0, ff)], dwg[w, :]) + dot_nt(d[r, pl.ds(ff, ff)], dwu[w, :])

    def terms(t):
        sl = lax.rem(t, 2)
        r = pl.ds(pl.multiple_of(t * R, R), R)

        @pl.when(t >= 2)
        def _():
            for p in range(3):
                reduce_copy(0, t - 2, p).wait_send()

        for p in range(3):
            w = pl.ds(pl.multiple_of(p * 2 * C + (1 - core) * C, C), C)
            s0[sl, p] = term(r, w).astype(jnp.bfloat16)
            reduce_copy(0, t, p).start()
        for p in range(3):
            w = pl.ds(pl.multiple_of(p * 2 * C + core * C, C), C)
            own[lax.rem(t, 4), p] = term(r, w)

    def weight_grads(u):
        sl = lax.rem(u, 2)

        for c in fetch_cols(u):
            c.wait()
        c = pl.ds(pl.multiple_of(u * TILE, TILE), TILE)
        dwg[c, :] = dot_tn(xb[sl], d[:, pl.ds(0, ff)]).astype(jnp.bfloat16)
        dwu[c, :] = dot_tn(xb[sl], d[:, pl.ds(ff, ff)]).astype(jnp.bfloat16)
        dwd[:, c] = jnp.dot(hid_t[...], yb[sl], preferred_element_type=jnp.float32).astype(jnp.bfloat16)

        @pl.when(u + 2 < units)
        def _():
            for c in fetch_cols(u + 2):
                c.start()

    def step(t, _):
        @pl.when(t < CHUNKS)
        def _():
            hidden_grads(t)

        @pl.when(t == 0)
        def _():
            weights[1].wait()
            weights[2].wait()
            for u in range(2):
                for c in fetch_cols(u):
                    c.start()

        @pl.when((t >= CHUNKS) & (2 * (t - CHUNKS) < units))
        def _():
            weight_grads(2 * (t - CHUNKS))

        live(t, 1, lambda k: reduce_step(1, k))
        live(t, 2, lambda k: reduce_step(2, k))
        live(t, 3, lambda k: reduce_step(3, k))
        live(t, 4, finish_step)

        @pl.when(t < CHUNKS)
        def _():
            terms(t)

        live(t, 5, lambda k: gather_step(1, k))
        live(t, 6, lambda k: gather_step(2, k))
        live(t, 7, lambda k: gather_step(3, k))

        @pl.when((t >= CHUNKS) & (2 * (t - CHUNKS) < units))
        def _():
            weight_grads(2 * (t - CHUNKS) + 1)

        return 0

    lax.fori_loop(0, CHUNKS + 7, step, 0)

    for stage in range(4):
        for k in (CHUNKS - 2, CHUNKS - 1):
            for p in range(3):
                reduce_copy(stage, k, p).wait_send()
    part = dx.at[pl.ds(0, 3), pl.ds(0, rows // 8 * 7), :]
    remote(part, part, ag_send, fwd_recv, mate).wait_send()
    half = dx.at[pl.ds(0, 3)]
    remote(half, half, fwd_send, fwd_recv, mate).wait()


def write_out(a, g, u, e, dx, dwg, dwu, dwd, sem):
    C = a.shape[2]
    copies = [pltpu.make_async_copy(a.at[j], dx.at[:, pl.ds(j * C, C)], sem.at[j]) for j in range(6)]
    copies += [pltpu.make_async_copy(s, t, sem.at[6 + j]) for j, (s, t) in enumerate(((g, dwg), (u, dwu), (e, dwd)))]
    for c in copies:
        c.start()
    for c in copies:
        c.wait()


def solution(mesh):
    def step(x, dy, gate, up, w_gate, w_up, w_down):
        rows, width = dy.shape
        ff = gate.shape[1]
        R, C, K = rows // CHUNKS, width // 6, CHUNKS
        bf, f32 = jnp.bfloat16, jnp.float32
        V, D = pltpu.VMEM, pltpu.SemaphoreType.DMA
        flops = 2 * rows * width * ff * 6
        hbm, vmem = pl.BlockSpec(memory_space=pl.ANY), pl.BlockSpec(memory_space=pltpu.VMEM)
        grads = pl.pallas_call(
            kernel,
            out_shape=(V((6, rows, C), bf), V((width, ff), bf), V((width, ff), bf), V((ff, width), bf)),
            in_specs=[hbm] * 7,
            out_specs=[vmem] * 4,
            scratch_shapes=[
                V((2, R, width), bf), V((2, R, ff), bf), V((2, R, ff), bf),
                V((rows, 2 * ff), bf), V((ff, rows), bf),
                V((4, 3, R, C), f32),
                V((2, 3, R, C), bf), V((2, 3, R // 2, C), bf), V((2, 3, R // 4, C), bf), V((2, 3, R // 8, C), bf),
                V((K, 3, R, C), bf), V((K, 3, R // 2, C), bf), V((K, 3, R // 4, C), bf), V((K, 3, R // 8, C), bf),
                V((2, rows, TILE), bf), V((2, rows, TILE), bf),
                D((3,)), D((3, 2)), D((2, 2)), D((4, 2, 3)), D((7, K, 3)), D, D, D,
            ],
            compiler_params=pltpu.CompilerParams(
                collective_id=0, has_side_effects=True, vmem_limit_bytes=44_000_000
            ),
            cost_estimate=pl.CostEstimate(flops=flops, bytes_accessed=60_000_000, transcendentals=rows * ff),
            name="mlp_grads",
        )(x, dy, gate, up, w_gate, w_up, w_down)
        return pl.pallas_call(
            write_out,
            out_shape=(
                jax.ShapeDtypeStruct((rows, width), bf),
                jax.ShapeDtypeStruct((width, ff), bf),
                jax.ShapeDtypeStruct((width, ff), bf),
                jax.ShapeDtypeStruct((ff, width), bf),
            ),
            in_specs=[vmem] * 4,
            out_specs=[hbm] * 4,
            scratch_shapes=[D((9,))],
            compiler_params=pltpu.CompilerParams(vmem_limit_bytes=1_000_000),
            name="write_out",
        )(*grads)

    tokens, columns, rows = P("dp", None), P(None, "tp"), P("tp", None)
    return jax.shard_map(
        step,
        mesh=mesh,
        in_specs=(tokens, tokens, P("dp", "tp"), P("dp", "tp"), columns, columns, rows),
        out_specs=(tokens, P("dp", "tp"), P("dp", "tp"), P(("dp", "tp"), None)),
        check_vma=False,
    )
```

```python
import functools

import jax
import jax.numpy as jnp
from jax import lax
from jax.experimental import pallas as pl
from jax.experimental.pallas import tpu as pltpu
from jax.sharding import PartitionSpec as P

MESH = pl.DeviceIdType.MESH
CHUNKS = 8
TILE = 256
LAGS = (0, 2, 4, 6, 8, 10, 12)
SLOTS = (2, 3, 4, 4)
ORDERS = ((8, 4, 2), (4, 2, 8), (2, 8, 4))


def dot_nt(a, b):
    return lax.dot_general(a, b, (((1,), (1,)), ((), ())), preferred_element_type=jnp.float32)


def dot_tn(a, b):
    return lax.dot_general(a, b, (((0,), (0,)), ((), ())), preferred_element_type=jnp.float32)


def kernel(
    x, dy, gate, up, wg, wu, wdn, dx, dwg, dwu, dwd,
    dyb, gb, ub, d, hid_t, own, s0, s1, s2, s3, r0, r1, r2, r3, xb, yb,
    w_sem, in_sem, xy_sem, s_sems, r_sems, ag_send, fwd_send, fwd_recv,
):
    rows, width = dy.shape
    ff = gate.shape[1]
    R = rows // CHUNKS
    C = width // 6
    dp = lax.axis_index("dp")
    me = lax.axis_index("tp")
    core = lax.rem(me, 2)
    mate = me + 1 - 2 * core
    bits = {s: lax.rem(me // s, 2) for s in (2, 4, 8)}
    peer = {s: me + (1 - 2 * bits[s]) * s for s in (2, 4, 8)}
    units = width // TILE

    def fetch(t):
        sl = lax.rem(t, 2)
        r = pl.ds(t * R, R)
        return (
            pltpu.make_async_copy(dy.at[r, :], dyb.at[sl], in_sem.at[0, sl]),
            pltpu.make_async_copy(gate.at[r, :], gb.at[sl], in_sem.at[1, sl]),
            pltpu.make_async_copy(up.at[r, :], ub.at[sl], in_sem.at[2, sl]),
        )

    def fetch_cols(u):
        sl = lax.rem(u, 2)
        c = pl.ds(pl.multiple_of(u * TILE, TILE), TILE)
        return (
            pltpu.make_async_copy(x.at[:, c], xb.at[sl], xy_sem.at[0, sl]),
            pltpu.make_async_copy(dy.at[:, c], yb.at[sl], xy_sem.at[1, sl]),
        )

    def down_half(h):
        r = pl.ds(h * (ff // 2), ff // 2)
        return pltpu.make_async_copy(wdn.at[r, :], dwd.at[r, :], w_sem.at[h])

    def columns_of(p, c):
        return pl.ds(pl.multiple_of(p * 2 * C + c * C, C), C)

    def weight_tile(i):
        w = columns_of(i % 3, core if i >= 3 else 1 - core)
        return (
            pltpu.make_async_copy(wg.at[w, :], dwg.at[w, :], w_sem.at[2 + i]),
            pltpu.make_async_copy(wu.at[w, :], dwu.at[w, :], w_sem.at[8 + i]),
        )

    down_half(0).start()
    for c in fetch(0):
        c.start()
    down_half(1).start()

    barrier = pltpu.get_barrier_semaphore()
    for to in (mate, peer[2], peer[4], peer[8]):
        pl.semaphore_signal(barrier, inc=1, device_id=(dp, to), device_id_type=MESH)
    pl.semaphore_wait(barrier, 4)
    for i in range(6):
        for c in weight_tile(i):
            c.start()

    def halves(p):
        n, kept, out = R, 0, []
        for s in ORDERS[p]:
            n //= 2
            out.append((n, kept + bits[s] * n, kept + (1 - bits[s]) * n, s))
            kept = kept + bits[s] * n
        return out

    def remote(src, dst, send, recv, to):
        return pltpu.make_async_remote_copy(
            src_ref=src, dst_ref=dst, send_sem=send, recv_sem=recv, device_id=(dp, to), device_id_type=MESH
        )

    sends, recvs = (s0, s1, s2, s3), (r0, r1, r2, r3)

    def reduce_copy(stage, k, p):
        sl = lax.rem(k, SLOTS[stage])
        to = mate if stage == 0 else peer[ORDERS[p][stage - 1]]
        return remote(
            sends[stage].at[sl, p],
            recvs[stage].at[k, p],
            s_sems.at[stage, sl, p],
            r_sems.at[stage, k, p],
            to,
        )

    def out_slice(k, p, off, n, c):
        row = pl.multiple_of(k * R + off, n)
        return dx.at[2 * p + c, pl.ds(row, n), :]

    def gather_copy(stage, k, p):
        n, kept, _, s = halves(p)[2 - stage]
        ref = out_slice(k, p, kept, n, core)
        return remote(ref, ref, ag_send, r_sems.at[4 + stage, k, p], peer[s])

    def forward_copy(k, p, off, n):
        ref = out_slice(k, p, off, n, core)
        return remote(ref, ref, fwd_send, fwd_recv, mate)

    def partial(k, p, stage, off, n):
        hs = halves(p)
        if stage == 1:
            total = own[CHUNKS, p]
        else:
            total = own[k, p, pl.ds(pl.multiple_of(off - hs[0][1], n), n), :]
        base = 0
        for i in range(stage):
            total += recvs[i][k, p, pl.ds(pl.multiple_of(off - base, n), n), :].astype(jnp.float32)
            base = hs[i][1] if i < 3 else base
        return total

    def reduce_step(stage, k):
        m = SLOTS[stage]
        sl = lax.rem(k, m)

        if not isinstance(k, int):

            @pl.when(k >= m)
            def _():
                for p in range(3):
                    reduce_copy(stage, k - m, p).wait_send()

        for p in range(3):
            n, _, sent, _ = halves(p)[stage - 1]
            reduce_copy(stage - 1, k, p).wait_recv()
            sends[stage][sl, p] = partial(k, p, stage, sent, n).astype(jnp.bfloat16)
            reduce_copy(stage, k, p).start()

    def finish_step(k):
        for p in range(3):
            n, kept, _, _ = halves(p)[2]
            reduce_copy(3, k, p).wait_recv()
            row = pl.multiple_of(k * R + kept, n)
            dx[2 * p + core, pl.ds(row, n), :] = partial(k, p, 4, kept, n).astype(jnp.bfloat16)
            gather_copy(0, k, p).start()
            forward_copy(k, p, kept, n).start()

    def gather_step(stage, k):
        for p in range(3):
            n, _, other, _ = halves(p)[3 - stage]
            gather_copy(stage - 1, k, p).wait_recv()
            if stage < 3:
                gather_copy(stage, k, p).start()
            forward_copy(k, p, other, n).start()

    def live(t, lag, f):
        k = t - lag

        @pl.when((k >= 0) & (k < CHUNKS))
        def _():
            f(k)

    def hidden_grads(t):
        sl = lax.rem(t, 2)
        @pl.when(t + 1 < CHUNKS)
        def _():
            for c in fetch(t + 1):
                c.start()

        for c in fetch(t):
            c.wait()
        r = pl.ds(pl.multiple_of(t * R, R), R)
        step = ff // 2
        for h in range(2):
            c = pl.ds(h * step, step)
            dh = dot_nt(dyb[sl], dwd[c, :])
            g = gb[sl, :, c].astype(jnp.float32)
            u = ub[sl, :, c].astype(jnp.float32)
            sg = jax.nn.sigmoid(g)
            silu = g * sg
            d[r, pl.ds(ff + h * step, step)] = (dh * silu).astype(jnp.bfloat16)
            d[r, c] = ((dh * u) * (sg * (1.0 + g * (1.0 - sg)))).astype(jnp.bfloat16)
            hid_t[c, r] = (silu * u).astype(jnp.bfloat16).T

    def term(r, w):
        return dot_nt(d[r, pl.ds(0, ff)], dwg[w, :]) + dot_nt(d[r, pl.ds(ff, ff)], dwu[w, :])

    def await_tiles(t, first):
        if isinstance(t, int):
            for i in range(first, first + 3):
                for c in weight_tile(i):
                    c.wait()

    def terms(t):
        sl = lax.rem(t, 2)
        r = pl.ds(pl.multiple_of(t * R, R), R)

        if not isinstance(t, int):

            @pl.when(t >= 2)
            def _():
                for p in range(3):
                    reduce_copy(0, t - 2, p).wait_send()

        await_tiles(t, 0)
        for p in range(3):
            w = columns_of(p, 1 - core)
            s0[sl, p] = term(r, w).astype(jnp.bfloat16)
            reduce_copy(0, t, p).start()
        await_tiles(t, 3)
        for p in range(3):
            w = columns_of(p, core)
            total = term(r, w)
            for i in range(2):
                kept = bits[ORDERS[p][0]] if i else 1 - bits[ORDERS[p][0]]
                own[kept * t + (1 - kept) * CHUNKS, p] = total[i * (R // 2) : (i + 1) * (R // 2)]

    def weight_grads(u):
        sl = lax.rem(u, 2)

        for c in fetch_cols(u):
            c.wait()
        c = pl.ds(pl.multiple_of(u * TILE, TILE), TILE)
        dwg[c, :] = dot_tn(xb[sl], d[:, pl.ds(0, ff)]).astype(jnp.bfloat16)
        dwu[c, :] = dot_tn(xb[sl], d[:, pl.ds(ff, ff)]).astype(jnp.bfloat16)
        dwd[:, c] = jnp.dot(hid_t[...], yb[sl], preferred_element_type=jnp.float32).astype(jnp.bfloat16)

        @pl.when(u + 2 < units)
        def _():
            for c in fetch_cols(u + 2):
                c.start()

    def step(t, _):
        @pl.when(t < CHUNKS)
        def _():
            hidden_grads(t)

        @pl.when(t == CHUNKS // 2)
        def _():
            for u in range(2):
                for c in fetch_cols(u):
                    c.start()

        @pl.when((t >= CHUNKS) & (2 * (t - CHUNKS) < units))
        def _():
            weight_grads(2 * (t - CHUNKS))

        live(t, LAGS[1], lambda k: reduce_step(2, k))
        live(t, LAGS[2], lambda k: reduce_step(3, k))
        live(t, LAGS[3], finish_step)

        @pl.when(t < CHUNKS)
        def _():
            terms(t)
            reduce_step(1, t)

        live(t, LAGS[4], lambda k: gather_step(1, k))
        live(t, LAGS[5], lambda k: gather_step(2, k))
        live(t, LAGS[6], lambda k: gather_step(3, k))

        @pl.when((t >= CHUNKS) & (2 * (t - CHUNKS) < units))
        def _():
            weight_grads(2 * (t - CHUNKS) + 1)

        return 0

    for h in range(2):
        down_half(h).wait()
    hidden_grads(0)
    terms(0)
    reduce_step(1, 0)
    lax.fori_loop(1, CHUNKS + LAGS[6], step, 0)

    for stage in range(4):
        for k in range(CHUNKS - SLOTS[stage], CHUNKS):
            for p in range(3):
                reduce_copy(stage, k, p).wait_send()
    part = dx.at[pl.ds(0, 3), pl.ds(0, rows // 8 * 7), :]
    remote(part, part, ag_send, fwd_recv, mate).wait_send()
    half = dx.at[pl.ds(0, 3)]
    remote(half, half, fwd_send, fwd_recv, mate).wait()


def write_out(a, g, u, e, dx, dwg, dwu, dwd, sem):
    C = a.shape[2]
    copies = [pltpu.make_async_copy(a.at[j], dx.at[:, pl.ds(j * C, C)], sem.at[j]) for j in range(6)]
    copies += [pltpu.make_async_copy(s, t, sem.at[6 + j]) for j, (s, t) in enumerate(((g, dwg), (u, dwu), (e, dwd)))]
    for c in copies:
        c.start()
    for c in copies:
        c.wait()


def solution(mesh):
    def step(x, dy, gate, up, w_gate, w_up, w_down):
        rows, width = dy.shape
        ff = gate.shape[1]
        R, C, K = rows // CHUNKS, width // 6, CHUNKS
        bf, f32 = jnp.bfloat16, jnp.float32
        V, D = pltpu.VMEM, pltpu.SemaphoreType.DMA
        flops = 2 * rows * width * ff * 6
        hbm, vmem = pl.BlockSpec(memory_space=pl.ANY), pl.BlockSpec(memory_space=pltpu.VMEM)
        grads = pl.pallas_call(
            kernel,
            out_shape=(V((6, rows, C), bf), V((width, ff), bf), V((width, ff), bf), V((ff, width), bf)),
            in_specs=[hbm] * 7,
            out_specs=[vmem] * 4,
            scratch_shapes=[
                V((2, R, width), bf), V((2, R, ff), bf), V((2, R, ff), bf),
                V((rows, 2 * ff), bf), V((ff, rows), bf),
                V((K + 1, 3, R // 2, C), f32),
                *(V((n, 3, R >> i, C), bf) for i, n in enumerate(SLOTS)),
                *(V((K, 3, R >> i, C), bf) for i in range(4)),
                V((2, rows, TILE), bf), V((2, rows, TILE), bf),
                D((14,)), D((3, 2)), D((2, 2)), D((4, max(SLOTS), 3)), D((7, K, 3)), D, D, D,
            ],
            compiler_params=pltpu.CompilerParams(
                collective_id=0, has_side_effects=True, vmem_limit_bytes=44_000_000
            ),
            cost_estimate=pl.CostEstimate(flops=flops, bytes_accessed=60_000_000, transcendentals=rows * ff),
            name="mlp_grads",
        )(x, dy, gate, up, w_gate, w_up, w_down)
        return pl.pallas_call(
            write_out,
            out_shape=(
                jax.ShapeDtypeStruct((rows, width), bf),
                jax.ShapeDtypeStruct((width, ff), bf),
                jax.ShapeDtypeStruct((width, ff), bf),
                jax.ShapeDtypeStruct((ff, width), bf),
            ),
            in_specs=[vmem] * 4,
            out_specs=[hbm] * 4,
            scratch_shapes=[D((9,))],
            compiler_params=pltpu.CompilerParams(vmem_limit_bytes=1_000_000),
            name="write_out",
        )(*grads)

    tokens, columns, rows = P("dp", None), P(None, "tp"), P("tp", None)
    return jax.shard_map(
        step,
        mesh=mesh,
        in_specs=(tokens, tokens, P("dp", "tp"), P("dp", "tp"), columns, columns, rows),
        out_specs=(tokens, P("dp", "tp"), P("dp", "tp"), P(("dp", "tp"), None)),
        check_vma=False,
    )
```

```python
import functools

import jax
import jax.numpy as jnp
from jax import lax
from jax.experimental import pallas as pl
from jax.experimental.pallas import tpu as pltpu
from jax.sharding import PartitionSpec as P

MESH = pl.DeviceIdType.MESH
CHUNKS = 8
TILE = 256
LAGS = (0, 2, 4, 6, 8, 10, 12)
SLOTS = (2, 3, 4, 4)
ORDERS = ((8, 4, 2), (4, 2, 8), (2, 8, 4))


def dot_nt(a, b):
    return lax.dot_general(a, b, (((1,), (1,)), ((), ())), preferred_element_type=jnp.float32)


def dot_tn(a, b):
    return lax.dot_general(a, b, (((0,), (0,)), ((), ())), preferred_element_type=jnp.float32)


def kernel(
    x, dy, gate, up, wg, wu, wdn, dx, dwg, dwu, dwd,
    dyb, gb, ub, d, hid_t, own, s0, s1, s2, s3, r0, r1, r2, r3, xb, yb,
    w_sem, in_sem, xy_sem, s_sems, r_sems, last_sems, ag_send, fwd_send, fwd_recv,
):
    rows, width = dy.shape
    ff = gate.shape[1]
    R = rows // CHUNKS
    C = width // 6
    dp = lax.axis_index("dp")
    me = lax.axis_index("tp")
    core = lax.rem(me, 2)
    mate = me + 1 - 2 * core
    bits = {s: lax.rem(me // s, 2) for s in (2, 4, 8)}
    peer = {s: me + (1 - 2 * bits[s]) * s for s in (2, 4, 8)}
    units = width // TILE

    def fetch(t):
        sl = lax.rem(t, 2)
        r = pl.ds(t * R, R)
        return (
            pltpu.make_async_copy(dy.at[r, :], dyb.at[sl], in_sem.at[0, sl]),
            pltpu.make_async_copy(gate.at[r, :], gb.at[sl], in_sem.at[1, sl]),
            pltpu.make_async_copy(up.at[r, :], ub.at[sl], in_sem.at[2, sl]),
        )

    def fetch_cols(u):
        sl = lax.rem(u, 2)
        c = pl.ds(pl.multiple_of(u * TILE, TILE), TILE)
        return (
            pltpu.make_async_copy(x.at[:, c], xb.at[sl], xy_sem.at[0, sl]),
            pltpu.make_async_copy(dy.at[:, c], yb.at[sl], xy_sem.at[1, sl]),
        )

    def down_half(h):
        r = pl.ds(h * (ff // 2), ff // 2)
        return pltpu.make_async_copy(wdn.at[r, :], dwd.at[r, :], w_sem.at[h])

    def columns_of(p, c):
        return pl.ds(pl.multiple_of(p * 2 * C + c * C, C), C)

    def weight_tile(i):
        w = columns_of(i % 3, core if i >= 3 else 1 - core)
        return (
            pltpu.make_async_copy(wg.at[w, :], dwg.at[w, :], w_sem.at[2 + i]),
            pltpu.make_async_copy(wu.at[w, :], dwu.at[w, :], w_sem.at[8 + i]),
        )

    down_half(0).start()
    for c in fetch(0):
        c.start()
    down_half(1).start()

    barrier = pltpu.get_barrier_semaphore()
    for to in (mate, peer[2], peer[4], peer[8]):
        pl.semaphore_signal(barrier, inc=1, device_id=(dp, to), device_id_type=MESH)
    pl.semaphore_wait(barrier, 4)
    for i in range(6):
        for c in weight_tile(i):
            c.start()

    def halves(p):
        n, kept, out = R, 0, []
        for s in ORDERS[p]:
            n //= 2
            out.append((n, kept + bits[s] * n, kept + (1 - bits[s]) * n, s))
            kept = kept + bits[s] * n
        return out

    def remote(src, dst, send, recv, to):
        return pltpu.make_async_remote_copy(
            src_ref=src, dst_ref=dst, send_sem=send, recv_sem=recv, device_id=(dp, to), device_id_type=MESH
        )

    sends, recvs = (s0, s1, s2, s3), (r0, r1, r2, r3)

    def reduce_copy(stage, k, p):
        sl = lax.rem(k, SLOTS[stage])
        to = mate if stage == 0 else peer[ORDERS[p][stage - 1]]
        return remote(
            sends[stage].at[sl, p],
            recvs[stage].at[k, p],
            s_sems.at[stage, sl, p],
            r_sems.at[stage, k, p],
            to,
        )

    def out_slice(k, p, off, n, c):
        row = pl.multiple_of(k * R + off, n)
        return dx.at[2 * p + c, pl.ds(row, n), :]

    def gather_copy(stage, k, p):
        n, kept, _, s = halves(p)[2 - stage]
        ref = out_slice(k, p, kept, n, core)
        return remote(ref, ref, ag_send, r_sems.at[4 + stage, k, p], peer[s])

    def last_copy(i, p):
        n, kept, _, a = halves(p)[0]
        ref = out_slice(CHUNKS - 1, p, kept + i * (n // 2), n // 2, core)
        recv = r_sems.at[6, CHUNKS - 1, p] if i else last_sems.at[p]
        return remote(ref, ref, ag_send, recv, peer[a])

    def forward_copy(k, p, off, n):
        ref = out_slice(k, p, off, n, core)
        return remote(ref, ref, fwd_send, fwd_recv, mate)

    def partial(k, p, stage, off, n):
        hs = halves(p)
        if stage == 1:
            total = own[CHUNKS, p]
        else:
            total = own[k, p, pl.ds(pl.multiple_of(off - hs[0][1], n), n), :]
        base = 0
        for i in range(stage):
            total += recvs[i][k, p, pl.ds(pl.multiple_of(off - base, n), n), :].astype(jnp.float32)
            base = hs[i][1] if i < 3 else base
        return total

    def reduce_step(stage, k):
        m = SLOTS[stage]
        sl = lax.rem(k, m)

        if not isinstance(k, int):

            @pl.when(k >= m)
            def _():
                for p in range(3):
                    reduce_copy(stage, k - m, p).wait_send()

        for p in range(3):
            n, _, sent, _ = halves(p)[stage - 1]
            reduce_copy(stage - 1, k, p).wait_recv()
            sends[stage][sl, p] = partial(k, p, stage, sent, n).astype(jnp.bfloat16)
            reduce_copy(stage, k, p).start()

    def finish_step(k):
        for p in range(3):
            n, kept, _, _ = halves(p)[2]
            reduce_copy(3, k, p).wait_recv()
            row = pl.multiple_of(k * R + kept, n)
            dx[2 * p + core, pl.ds(row, n), :] = partial(k, p, 4, kept, n).astype(jnp.bfloat16)
            gather_copy(0, k, p).start()
            forward_copy(k, p, kept, n).start()

    def gather_step(stage, k):
        for p in range(3):
            n, _, other, _ = halves(p)[3 - stage]
            gather_copy(stage - 1, k, p).wait_recv()
            if stage < 3:
                gather_copy(stage, k, p).start()
            forward_copy(k, p, other, n).start()

    def live(t, lag, f):
        k = t - lag

        @pl.when((k >= 0) & (k < CHUNKS))
        def _():
            f(k)

    def hidden_grads(t):
        sl = lax.rem(t, 2)
        @pl.when(t + 1 < CHUNKS)
        def _():
            for c in fetch(t + 1):
                c.start()

        for c in fetch(t):
            c.wait()
        r = pl.ds(pl.multiple_of(t * R, R), R)
        step = ff // 2
        back = dot_nt(dyb[sl], dwd[...])
        for h in range(2):
            c = pl.ds(h * step, step)
            dh = back[:, h * step : (h + 1) * step]
            g = gb[sl, :, c].astype(jnp.float32)
            u = ub[sl, :, c].astype(jnp.float32)
            sg = jax.nn.sigmoid(g)
            silu = g * sg
            d[r, pl.ds(ff + h * step, step)] = (dh * silu).astype(jnp.bfloat16)
            d[r, c] = ((dh * u) * (sg * (1.0 + g * (1.0 - sg)))).astype(jnp.bfloat16)
            hid_t[c, r] = (silu * u).astype(jnp.bfloat16).T

    def term(r, w):
        return dot_nt(d[r, pl.ds(0, ff)], dwg[w, :]) + dot_nt(d[r, pl.ds(ff, ff)], dwu[w, :])

    def await_tiles(t, first):
        if isinstance(t, int):
            for i in range(first, first + 3):
                for c in weight_tile(i):
                    c.wait()

    def terms(t):
        sl = lax.rem(t, 2)
        r = pl.ds(pl.multiple_of(t * R, R), R)

        if not isinstance(t, int):

            @pl.when(t >= 2)
            def _():
                for p in range(3):
                    reduce_copy(0, t - 2, p).wait_send()

        await_tiles(t, 0)
        for p in range(3):
            w = columns_of(p, 1 - core)
            s0[sl, p] = term(r, w).astype(jnp.bfloat16)
            reduce_copy(0, t, p).start()
        await_tiles(t, 3)
        for p in range(3):
            w = columns_of(p, core)
            total = term(r, w)
            for i in range(2):
                kept = bits[ORDERS[p][0]] if i else 1 - bits[ORDERS[p][0]]
                own[kept * t + (1 - kept) * CHUNKS, p] = total[i * (R // 2) : (i + 1) * (R // 2)]

    def weight_grads(u):
        sl = lax.rem(u, 2)

        for c in fetch_cols(u):
            c.wait()
        c = pl.ds(pl.multiple_of(u * TILE, TILE), TILE)
        dwg[c, :] = dot_tn(xb[sl], d[:, pl.ds(0, ff)]).astype(jnp.bfloat16)
        dwu[c, :] = dot_tn(xb[sl], d[:, pl.ds(ff, ff)]).astype(jnp.bfloat16)
        dwd[:, c] = jnp.dot(hid_t[...], yb[sl], preferred_element_type=jnp.float32).astype(jnp.bfloat16)

        @pl.when(u + 2 < units)
        def _():
            for c in fetch_cols(u + 2):
                c.start()

    def step(t, _):
        @pl.when(t < CHUNKS)
        def _():
            hidden_grads(t)

        @pl.when(t == CHUNKS // 2)
        def _():
            for u in range(2):
                for c in fetch_cols(u):
                    c.start()

        @pl.when((t >= CHUNKS) & (2 * (t - CHUNKS) < units))
        def _():
            weight_grads(2 * (t - CHUNKS))

        live(t, LAGS[1], lambda k: reduce_step(2, k))
        live(t, LAGS[2], lambda k: reduce_step(3, k))
        live(t, LAGS[3], finish_step)

        @pl.when(t < CHUNKS)
        def _():
            terms(t)
            reduce_step(1, t)

        live(t, LAGS[4], lambda k: gather_step(1, k))
        live(t, LAGS[5], lambda k: gather_step(2, k))
        live(t, LAGS[6], lambda k: gather_step(3, k))

        @pl.when((t >= CHUNKS) & (2 * (t - CHUNKS) < units))
        def _():
            weight_grads(2 * (t - CHUNKS) + 1)

        return 0

    for h in range(2):
        down_half(h).wait()
    hidden_grads(0)
    terms(0)
    reduce_step(1, 0)
    end = CHUNKS - 1 + LAGS[5]
    lax.fori_loop(1, end, step, 0)
    for p in range(3):
        n, _, other, _ = halves(p)[1]
        gather_copy(1, CHUNKS - 1, p).wait_recv()
        last_copy(0, p).start()
        last_copy(1, p).start()
        forward_copy(CHUNKS - 1, p, other, n).start()
    for k in range(end - LAGS[6], CHUNKS - 1):
        gather_step(3, k)
    for i in range(2):
        for p in range(3):
            n, _, other, _ = halves(p)[0]
            last_copy(i, p).wait_recv()
            forward_copy(CHUNKS - 1, p, other + i * (n // 2), n // 2).start()

    for stage in range(4):
        for k in range(CHUNKS - SLOTS[stage], CHUNKS):
            for p in range(3):
                reduce_copy(stage, k, p).wait_send()
    part = dx.at[pl.ds(0, 3), pl.ds(0, rows // 8 * 7), :]
    remote(part, part, ag_send, fwd_recv, mate).wait_send()
    half = dx.at[pl.ds(0, 3)]
    remote(half, half, fwd_send, fwd_recv, mate).wait()


def write_out(a, g, u, e, dx, dwg, dwu, dwd, sem):
    C = a.shape[2]
    copies = [pltpu.make_async_copy(a.at[j], dx.at[:, pl.ds(j * C, C)], sem.at[j]) for j in range(6)]
    copies += [pltpu.make_async_copy(s, t, sem.at[6 + j]) for j, (s, t) in enumerate(((g, dwg), (u, dwu), (e, dwd)))]
    for c in copies:
        c.start()
    for c in copies:
        c.wait()


def solution(mesh):
    def step(x, dy, gate, up, w_gate, w_up, w_down):
        rows, width = dy.shape
        ff = gate.shape[1]
        R, C, K = rows // CHUNKS, width // 6, CHUNKS
        bf, f32 = jnp.bfloat16, jnp.float32
        V, D = pltpu.VMEM, pltpu.SemaphoreType.DMA
        flops = 2 * rows * width * ff * 6
        hbm, vmem = pl.BlockSpec(memory_space=pl.ANY), pl.BlockSpec(memory_space=pltpu.VMEM)
        grads = pl.pallas_call(
            kernel,
            out_shape=(V((6, rows, C), bf), V((width, ff), bf), V((width, ff), bf), V((ff, width), bf)),
            in_specs=[hbm] * 7,
            out_specs=[vmem] * 4,
            scratch_shapes=[
                V((2, R, width), bf), V((2, R, ff), bf), V((2, R, ff), bf),
                V((rows, 2 * ff), bf), V((ff, rows), bf),
                V((K + 1, 3, R // 2, C), f32),
                *(V((n, 3, R >> i, C), bf) for i, n in enumerate(SLOTS)),
                *(V((K, 3, R >> i, C), bf) for i in range(4)),
                V((2, rows, TILE), bf), V((2, rows, TILE), bf),
                D((14,)), D((3, 2)), D((2, 2)), D((4, max(SLOTS), 3)), D((7, K, 3)), D((3,)), D, D, D,
            ],
            compiler_params=pltpu.CompilerParams(
                collective_id=0, has_side_effects=True, vmem_limit_bytes=44_000_000
            ),
            cost_estimate=pl.CostEstimate(flops=flops, bytes_accessed=60_000_000, transcendentals=rows * ff),
            name="mlp_grads",
        )(x, dy, gate, up, w_gate, w_up, w_down)
        return pl.pallas_call(
            write_out,
            out_shape=(
                jax.ShapeDtypeStruct((rows, width), bf),
                jax.ShapeDtypeStruct((width, ff), bf),
                jax.ShapeDtypeStruct((width, ff), bf),
                jax.ShapeDtypeStruct((ff, width), bf),
            ),
            in_specs=[vmem] * 4,
            out_specs=[hbm] * 4,
            scratch_shapes=[D((9,))],
            compiler_params=pltpu.CompilerParams(vmem_limit_bytes=1_000_000),
            name="write_out",
        )(*grads)

    tokens, columns, rows = P("dp", None), P(None, "tp"), P("tp", None)
    return jax.shard_map(
        step,
        mesh=mesh,
        in_specs=(tokens, tokens, P("dp", "tp"), P("dp", "tp"), columns, columns, rows),
        out_specs=(tokens, P("dp", "tp"), P("dp", "tp"), P(("dp", "tp"), None)),
        check_vma=False,
    )
```

```python
import functools

import jax
import jax.numpy as jnp
from jax import lax
from jax.experimental import pallas as pl
from jax.experimental.pallas import tpu as pltpu
from jax.sharding import PartitionSpec as P

MESH = pl.DeviceIdType.MESH
CHUNKS = 8
TILE = 256
LAGS = (0, 2, 4, 6, 8, 10, 12)
SLOTS = (2, 3, 4, 4)
ORDERS = ((8, 4, 2), (4, 2, 8), (2, 8, 4))


def dot_nt(a, b):
    return lax.dot_general(a, b, (((1,), (1,)), ((), ())), preferred_element_type=jnp.float32)


def dot_tn(a, b):
    return lax.dot_general(a, b, (((0,), (0,)), ((), ())), preferred_element_type=jnp.float32)


def kernel(
    x, dy, gate, up, wg, wu, wdn, dx, dwg, dwu, dwd,
    dyb, gb, ub, d, hid_t, own, s0, s1, s2, s3, r0, r1, r2, r3, xb, yb,
    w_sem, in_sem, xy_sem, s_sems, r_sems, last_sems, ag_send, fwd_send, fwd_recv,
):
    rows, width = dy.shape
    ff = gate.shape[1]
    R = rows // CHUNKS
    C = width // 6
    dp = lax.axis_index("dp")
    me = lax.axis_index("tp")
    core = lax.rem(me, 2)
    mate = me + 1 - 2 * core
    bits = {s: lax.rem(me // s, 2) for s in (2, 4, 8)}
    peer = {s: me + (1 - 2 * bits[s]) * s for s in (2, 4, 8)}
    units = width // TILE

    def fetch(t):
        sl = lax.rem(t, 2)
        r = pl.ds(t * R, R)
        return (
            pltpu.make_async_copy(dy.at[r, :], dyb.at[sl], in_sem.at[0, sl]),
            pltpu.make_async_copy(gate.at[r, :], gb.at[sl], in_sem.at[1, sl]),
            pltpu.make_async_copy(up.at[r, :], ub.at[sl], in_sem.at[2, sl]),
        )

    def fetch_cols(u):
        sl = lax.rem(u, 2)
        c = pl.ds(pl.multiple_of(u * TILE, TILE), TILE)
        return (
            pltpu.make_async_copy(x.at[:, c], xb.at[sl], xy_sem.at[0, sl]),
            pltpu.make_async_copy(dy.at[:, c], yb.at[sl], xy_sem.at[1, sl]),
        )

    def down_half(h):
        r = pl.ds(h * (ff // 2), ff // 2)
        return pltpu.make_async_copy(wdn.at[r, :], dwd.at[r, :], w_sem.at[h])

    def columns_of(p, c):
        return pl.ds(pl.multiple_of(p * 2 * C + c * C, C), C)

    def weight_tile(i):
        w = columns_of(i % 3, core if i >= 3 else 1 - core)
        return (
            pltpu.make_async_copy(wg.at[w, :], dwg.at[w, :], w_sem.at[2 + i]),
            pltpu.make_async_copy(wu.at[w, :], dwu.at[w, :], w_sem.at[8 + i]),
        )

    down_half(0).start()
    for c in fetch(0):
        c.start()
    down_half(1).start()

    barrier = pltpu.get_barrier_semaphore()
    for to in (mate, peer[2], peer[4], peer[8]):
        pl.semaphore_signal(barrier, inc=1, device_id=(dp, to), device_id_type=MESH)
    pl.semaphore_wait(barrier, 4)
    for i in range(6):
        for c in weight_tile(i):
            c.start()

    def halves(p):
        n, kept, out = R, 0, []
        for s in ORDERS[p]:
            n //= 2
            out.append((n, kept + bits[s] * n, kept + (1 - bits[s]) * n, s))
            kept = kept + bits[s] * n
        return out

    def remote(src, dst, send, recv, to):
        return pltpu.make_async_remote_copy(
            src_ref=src, dst_ref=dst, send_sem=send, recv_sem=recv, device_id=(dp, to), device_id_type=MESH
        )

    sends, recvs = (s0, s1, s2, s3), (r0, r1, r2, r3)

    def reduce_copy(stage, k, p):
        sl = lax.rem(k, SLOTS[stage])
        to = mate if stage == 0 else peer[ORDERS[p][stage - 1]]
        return remote(
            sends[stage].at[sl, p],
            recvs[stage].at[k, p],
            s_sems.at[stage, sl, p],
            r_sems.at[stage, k, p],
            to,
        )

    def out_slice(k, p, off, n, c):
        row = pl.multiple_of(k * R + off, n)
        return dx.at[2 * p + c, pl.ds(row, n), :]

    def gather_copy(stage, k, p):
        n, kept, _, s = halves(p)[2 - stage]
        ref = out_slice(k, p, kept, n, core)
        return remote(ref, ref, ag_send, r_sems.at[4 + stage, k, p], peer[s])

    def last_copy(i, p):
        n, kept, _, a = halves(p)[0]
        ref = out_slice(CHUNKS - 1, p, kept + i * (n // 2), n // 2, core)
        recv = r_sems.at[6, CHUNKS - 1, p] if i else last_sems.at[p]
        return remote(ref, ref, ag_send, recv, peer[a])

    def forward_copy(k, p, off, n):
        ref = out_slice(k, p, off, n, core)
        return remote(ref, ref, fwd_send, fwd_recv, mate)

    def partial(k, p, stage, off, n):
        hs = halves(p)
        if stage == 1:
            total = own[CHUNKS, p]
        else:
            total = own[k, p, pl.ds(pl.multiple_of(off - hs[0][1], n), n), :]
        base = 0
        for i in range(stage):
            total += recvs[i][k, p, pl.ds(pl.multiple_of(off - base, n), n), :].astype(jnp.float32)
            base = hs[i][1] if i < 3 else base
        return total

    def reduce_step(stage, k):
        m = SLOTS[stage]
        sl = lax.rem(k, m)

        if not isinstance(k, int):

            @pl.when(k >= m)
            def _():
                for p in range(3):
                    reduce_copy(stage, k - m, p).wait_send()

        for p in range(3):
            n, _, sent, _ = halves(p)[stage - 1]
            reduce_copy(stage - 1, k, p).wait_recv()
            sends[stage][sl, p] = partial(k, p, stage, sent, n).astype(jnp.bfloat16)
            reduce_copy(stage, k, p).start()

    def finish_step(k):
        for p in range(3):
            n, kept, _, _ = halves(p)[2]
            reduce_copy(3, k, p).wait_recv()
            row = pl.multiple_of(k * R + kept, n)
            dx[2 * p + core, pl.ds(row, n), :] = partial(k, p, 4, kept, n).astype(jnp.bfloat16)
            gather_copy(0, k, p).start()
            forward_copy(k, p, kept, n).start()

    def gather_step(stage, k):
        for p in range(3):
            n, _, other, _ = halves(p)[3 - stage]
            gather_copy(stage - 1, k, p).wait_recv()
            if stage < 3:
                gather_copy(stage, k, p).start()
            forward_copy(k, p, other, n).start()

    def live(t, lag, f):
        k = t - lag

        @pl.when((k >= 0) & (k < CHUNKS))
        def _():
            f(k)

    def hidden_grads(t):
        sl = lax.rem(t, 2)
        @pl.when(t + 1 < CHUNKS)
        def _():
            for c in fetch(t + 1):
                c.start()

        for c in fetch(t):
            c.wait()
        r = pl.ds(pl.multiple_of(t * R, R), R)
        step = ff // 2
        back = dot_nt(dyb[sl], dwd[...])
        for h in range(2):
            c = pl.ds(h * step, step)
            dh = back[:, h * step : (h + 1) * step]
            g = gb[sl, :, c].astype(jnp.float32)
            u = ub[sl, :, c].astype(jnp.float32)
            sg = jax.nn.sigmoid(g)
            silu = g * sg
            d[r, pl.ds(ff + h * step, step)] = (dh * silu).astype(jnp.bfloat16)
            d[r, c] = ((dh * u) * (sg * (1.0 + g * (1.0 - sg)))).astype(jnp.bfloat16)
            hid_t[c, r] = (silu * u).astype(jnp.bfloat16).T

    def term(r, w):
        return dot_nt(d[r, pl.ds(0, ff)], dwg[w, :]) + dot_nt(d[r, pl.ds(ff, ff)], dwu[w, :])

    def await_tiles(t, first):
        if isinstance(t, int):
            for i in range(first, first + 3):
                for c in weight_tile(i):
                    c.wait()

    def terms(t):
        sl = lax.rem(t, 2)
        r = pl.ds(pl.multiple_of(t * R, R), R)

        if not isinstance(t, int):

            @pl.when(t >= 2)
            def _():
                for p in range(3):
                    reduce_copy(0, t - 2, p).wait_send()

        await_tiles(t, 0)
        for p in range(3):
            w = columns_of(p, 1 - core)
            s0[sl, p] = term(r, w).astype(jnp.bfloat16)
            reduce_copy(0, t, p).start()
    def own_terms(t):
        r = pl.ds(pl.multiple_of(t * R, R), R)
        await_tiles(t, 3)
        for p in range(3):
            w = columns_of(p, core)
            total = term(r, w)
            for i in range(2):
                kept = bits[ORDERS[p][0]] if i else 1 - bits[ORDERS[p][0]]
                own[kept * t + (1 - kept) * CHUNKS, p] = total[i * (R // 2) : (i + 1) * (R // 2)]

    def weight_grads(u):
        sl = lax.rem(u, 2)

        for c in fetch_cols(u):
            c.wait()
        c = pl.ds(pl.multiple_of(u * TILE, TILE), TILE)
        dwg[c, :] = dot_tn(xb[sl], d[:, pl.ds(0, ff)]).astype(jnp.bfloat16)
        dwu[c, :] = dot_tn(xb[sl], d[:, pl.ds(ff, ff)]).astype(jnp.bfloat16)
        dwd[:, c] = jnp.dot(hid_t[...], yb[sl], preferred_element_type=jnp.float32).astype(jnp.bfloat16)

        @pl.when(u + 2 < units)
        def _():
            for c in fetch_cols(u + 2):
                c.start()

    def step(t, _):
        @pl.when(t < CHUNKS)
        def _():
            hidden_grads(t)

        @pl.when(t == CHUNKS // 2)
        def _():
            for u in range(2):
                for c in fetch_cols(u):
                    c.start()

        @pl.when((t >= CHUNKS) & (2 * (t - CHUNKS) < units))
        def _():
            weight_grads(2 * (t - CHUNKS))

        @pl.when(t < CHUNKS)
        def _():
            terms(t)

        live(t, LAGS[1], lambda k: reduce_step(2, k))
        live(t, LAGS[2], lambda k: reduce_step(3, k))
        live(t, LAGS[3], finish_step)

        @pl.when(t < CHUNKS)
        def _():
            own_terms(t)
            reduce_step(1, t)

        live(t, LAGS[4], lambda k: gather_step(1, k))
        live(t, LAGS[5], lambda k: gather_step(2, k))
        live(t, LAGS[6], lambda k: gather_step(3, k))

        @pl.when((t >= CHUNKS) & (2 * (t - CHUNKS) < units))
        def _():
            weight_grads(2 * (t - CHUNKS) + 1)

        return 0

    for h in range(2):
        down_half(h).wait()
    hidden_grads(0)
    terms(0)
    own_terms(0)
    reduce_step(1, 0)
    end = CHUNKS - 1 + LAGS[5]
    lax.fori_loop(1, end, step, 0)
    for p in range(3):
        n, _, other, _ = halves(p)[1]
        gather_copy(1, CHUNKS - 1, p).wait_recv()
        last_copy(0, p).start()
        last_copy(1, p).start()
        forward_copy(CHUNKS - 1, p, other, n).start()
    for k in range(end - LAGS[6], CHUNKS - 1):
        gather_step(3, k)
    for i in range(2):
        for p in range(3):
            n, _, other, _ = halves(p)[0]
            last_copy(i, p).wait_recv()
            forward_copy(CHUNKS - 1, p, other + i * (n // 2), n // 2).start()

    for stage in range(4):
        for k in range(CHUNKS - SLOTS[stage], CHUNKS):
            for p in range(3):
                reduce_copy(stage, k, p).wait_send()
    part = dx.at[pl.ds(0, 3), pl.ds(0, rows // 8 * 7), :]
    remote(part, part, ag_send, fwd_recv, mate).wait_send()
    half = dx.at[pl.ds(0, 3)]
    remote(half, half, fwd_send, fwd_recv, mate).wait()


def write_out(a, g, u, e, dx, dwg, dwu, dwd, sem):
    C = a.shape[2]
    copies = [pltpu.make_async_copy(a.at[j], dx.at[:, pl.ds(j * C, C)], sem.at[j]) for j in range(6)]
    copies += [pltpu.make_async_copy(s, t, sem.at[6 + j]) for j, (s, t) in enumerate(((g, dwg), (u, dwu), (e, dwd)))]
    for c in copies:
        c.start()
    for c in copies:
        c.wait()


def solution(mesh):
    def step(x, dy, gate, up, w_gate, w_up, w_down):
        rows, width = dy.shape
        ff = gate.shape[1]
        R, C, K = rows // CHUNKS, width // 6, CHUNKS
        bf, f32 = jnp.bfloat16, jnp.float32
        V, D = pltpu.VMEM, pltpu.SemaphoreType.DMA
        flops = 2 * rows * width * ff * 6
        hbm, vmem = pl.BlockSpec(memory_space=pl.ANY), pl.BlockSpec(memory_space=pltpu.VMEM)
        grads = pl.pallas_call(
            kernel,
            out_shape=(V((6, rows, C), bf), V((width, ff), bf), V((width, ff), bf), V((ff, width), bf)),
            in_specs=[hbm] * 7,
            out_specs=[vmem] * 4,
            scratch_shapes=[
                V((2, R, width), bf), V((2, R, ff), bf), V((2, R, ff), bf),
                V((rows, 2 * ff), bf), V((ff, rows), bf),
                V((K + 1, 3, R // 2, C), f32),
                *(V((n, 3, R >> i, C), bf) for i, n in enumerate(SLOTS)),
                *(V((K, 3, R >> i, C), bf) for i in range(4)),
                V((2, rows, TILE), bf), V((2, rows, TILE), bf),
                D((14,)), D((3, 2)), D((2, 2)), D((4, max(SLOTS), 3)), D((7, K, 3)), D((3,)), D, D, D,
            ],
            compiler_params=pltpu.CompilerParams(
                collective_id=0, has_side_effects=True, vmem_limit_bytes=44_000_000
            ),
            cost_estimate=pl.CostEstimate(flops=flops, bytes_accessed=60_000_000, transcendentals=rows * ff),
            name="mlp_grads",
        )(x, dy, gate, up, w_gate, w_up, w_down)
        return pl.pallas_call(
            write_out,
            out_shape=(
                jax.ShapeDtypeStruct((rows, width), bf),
                jax.ShapeDtypeStruct((width, ff), bf),
                jax.ShapeDtypeStruct((width, ff), bf),
                jax.ShapeDtypeStruct((ff, width), bf),
            ),
            in_specs=[vmem] * 4,
            out_specs=[hbm] * 4,
            scratch_shapes=[D((9,))],
            compiler_params=pltpu.CompilerParams(vmem_limit_bytes=1_000_000),
            name="write_out",
        )(*grads)

    tokens, columns, rows = P("dp", None), P(None, "tp"), P("tp", None)
    return jax.shard_map(
        step,
        mesh=mesh,
        in_specs=(tokens, tokens, P("dp", "tp"), P("dp", "tp"), columns, columns, rows),
        out_specs=(tokens, P("dp", "tp"), P("dp", "tp"), P(("dp", "tp"), None)),
        check_vma=False,
    )
```
